32 devices in a mesh: dp: 4 (over z), table: 8 (over y, x, core).
Axes of the slice: x: 2, y: 2, z: 4, core: 2. Of those that a mesh axis runs over, the one named last changes fastest.
Arguments:
- table: bfloat16 [4096, 256], P('table'), may hold values from -6 to 6
- weights: bfloat16 [2, 6, 256, 256], replicated, may hold values from -0.375 to 0.375
- fetch_rows: int32 [4, 8, 8, 32], P('dp', 'table'), may hold values from 0 to 511
- fetch_count: int32 [4, 8, 8], P('dp', 'table'), may hold values from 1 to 32, as said below
- first_self: int32 [4, 8, 256], P('dp', 'table'), may hold values from 0 to 255, as said below
- first_edges: int32 [4, 8, 5, 256, 4], P('dp', 'table'), may hold values from 0 to 255, as said below
- first_degree: int32 [4, 8, 5, 256], P('dp', 'table'), may hold values from 1 to 4
- second_self: int32 [4, 8, 128], P('dp', 'table'), may hold values from 0 to 255
- second_edges: int32 [4, 8, 5, 128, 4], P('dp', 'table'), may hold values from 0 to 255
- second_degree: int32 [4, 8, 5, 128], P('dp', 'table'), may hold values from 1 to 4
- cotangent: bfloat16 [4, 8, 128, 256], P('dp', 'table'), may hold values from -6 to 6
Outputs:
- node_out: bfloat16 [4, 8, 128, 256], P('dp', 'table')
- weight_grad: bfloat16 [2, 6, 256, 256], replicated
- table_grad: float32 [8, 512, 256], P('table', 'dp')
The draws below stay inside these ranges and needn't reach their ends.
Inputs may be any that keep to these rules, and one draw needn't show every extreme that they name: Minibatch (i, j) uses the first fetch_count[i, j, k] slots for shard k; for each i one shard is given all 32 slots by every minibatch of that i, and every other count is at most 16. `fetch_rows`: slots past the count hold arbitrary row numbers. `first_self`: every entry is a live slot k * 32 + c with c < fetch_count of shard k. `first_edges`: every entry, used or not, is a live slot k * 32 + c with c < fetch_count of shard k.
All inputs are finite; a program needn't handle non-finite values.
Results may differ from the reference program's by a relative error of at most 0.0057.
Values may be sent and summed in bfloat16 or wider, within the bound.
A program may use at most 64 MiB of HBM per device.

```python
import jax
import jax.numpy as jnp
from jax import lax

D = 256
R = 5
FAN = 4
ROWS_DEV = 512
CAP = 32
B2 = 128
B1 = 256
SLOTS = 256
VOCAB = 4096
SEEDS = 4096
N_DP = 4
N_TABLE = 8


def owner_counts(key):
    layout = (N_DP, N_TABLE, N_TABLE)
    lowest = max(1, CAP // 8)
    drawn = jax.random.randint(jax.random.fold_in(key, 11), layout, lowest, CAP // 2 + 1)
    hottest = jax.random.randint(jax.random.fold_in(key, 12), (N_DP, 1, 1), 0, N_TABLE)
    owners = lax.broadcasted_iota(jnp.int32, layout, 2)
    return jnp.where(owners == hottest, CAP, drawn).astype(jnp.int32)


def live_slots(key, extent, salt):
    counts = owner_counts(key)
    owners = jax.random.randint(jax.random.fold_in(key, salt), extent, 0, N_TABLE)
    flatwise = owners.reshape(N_DP, N_TABLE, -1)
    limits = jnp.take_along_axis(counts, flatwise, axis=2).reshape(extent)
    within = jax.random.randint(jax.random.fold_in(key, salt + 1), extent, 0, limits)
    return (owners * CAP + within).astype(jnp.int32)


def draw_fetch_count(key, part):
    return owner_counts(key)


def draw_first_self(key, part):
    return live_slots(key, (N_DP, N_TABLE, B1), 21)


def draw_first_edges(key, part):
    return live_slots(key, (N_DP, N_TABLE, R, B1, FAN), 31)


def plant(values, own_key, smallest, high):
    longest = values.shape.index(max(values.shape))
    spots = []
    for shift in (0, 1):
        where = [jax.random.randint(jax.random.fold_in(own_key, axis), (), 0, length) for axis, length in enumerate(values.shape)]
        where[longest] = (where[longest] + shift) % values.shape[longest]
        spots.append(tuple(where))
    return values.at[spots[0]].set(smallest).at[spots[1]].set(high)


def steps_of(key, shape, split, low, high):
    loudness = 1.0
    for dim, blocks in split:
        heights = jax.random.uniform(jax.random.fold_in(jax.random.fold_in(key, 6), dim), (blocks,), jnp.float32, low / len(split), high / len(split))
        loudness = loudness * jnp.repeat(jnp.exp(heights), shape[dim] // blocks).reshape((-1,) + (1,) * (len(shape) - 1 - dim))
    return loudness


def centred(own_key, shape, width, limit, split=(), kind=jnp.bfloat16):
    entries = jax.random.normal(own_key, shape, jnp.float32) * width
    if len(split) > 0:
        entries = steps_of(own_key, shape, split, -0.22, 0.18) * entries
    return jnp.clip(entries, min=-limit, max=limit).astype(kind)


def setup_inputs(seed: int = 0) -> dict:
    keys = jax.random.split(jax.random.key(seed), 12)
    table = centred(keys[0], (VOCAB, D), 1.0, 6.0, ((0, 8),))
    weights = centred(keys[1], (2, R + 1, D, D), D ** -0.5, 0.375)
    fetch_rows = plant(jax.random.randint(keys[2], (N_DP, N_TABLE, N_TABLE, CAP), 0, ROWS_DEV), jax.random.fold_in(keys[2], 1), 0, ROWS_DEV - 1).astype(jnp.int32)
    fetch_count = draw_fetch_count(jax.random.fold_in(keys[11], 71), 0)
    first_self = draw_first_self(jax.random.fold_in(keys[11], 71), 0)
    first_edges = draw_first_edges(jax.random.fold_in(keys[11], 71), 0)
    first_degree = plant(jax.random.randint(keys[6], (N_DP, N_TABLE, R, B1), 1, FAN + 1), jax.random.fold_in(keys[6], 1), 1, FAN).astype(jnp.int32)
    second_self = plant(jax.random.randint(keys[7], (N_DP, N_TABLE, B2), 0, B1), jax.random.fold_in(keys[7], 1), 0, B1 - 1).astype(jnp.int32)
    second_edges = plant(jax.random.randint(keys[8], (N_DP, N_TABLE, R, B2, FAN), 0, B1), jax.random.fold_in(keys[8], 1), 0, B1 - 1).astype(jnp.int32)
    second_degree = plant(jax.random.randint(keys[9], (N_DP, N_TABLE, R, B2), 1, FAN + 1), jax.random.fold_in(keys[9], 1), 1, FAN).astype(jnp.int32)
    cotangent = centred(keys[10], (N_DP, N_TABLE, B2, D), 1.0, 6.0, ((0, 4), (1, 8)))
    return dict(table=table, weights=weights, fetch_rows=fetch_rows, fetch_count=fetch_count, first_self=first_self, first_edges=first_edges, first_degree=first_degree, second_self=second_self, second_edges=second_edges, second_degree=second_degree, cotangent=cotangent)


def aggregate(features, edges, degrees):

    def single(bundle):
        indices, degree = bundle
        within = lax.broadcasted_iota(jnp.int32, indices.shape, 1) < degree[:, None]
        picked = jnp.where(within[:, :, None], features[indices], jnp.zeros((), features.dtype))
        summed = lax.optimization_barrier(jnp.sum(picked.astype(jnp.float32), axis=1))
        return (summed / degree[:, None].astype(jnp.float32)).astype(jnp.bfloat16)
    return lax.map(single, (edges, degrees))

def spread_back(grads, edges, degrees, height):

    def single(running, bundle):
        part_grad, indices, degree = bundle
        within = lax.broadcasted_iota(jnp.int32, indices.shape, 1) < degree[:, None]
        scaled = part_grad / degree[:, None].astype(part_grad.dtype)
        placed = jnp.where(within[:, :, None], scaled[:, None, :], jnp.zeros((), part_grad.dtype))
        return (running.at[indices.reshape(-1)].add(placed.reshape(-1, part_grad.shape[-1])), None)
    initial = jnp.zeros((height, grads.shape[-1]), grads.dtype)
    result, ignored = lax.scan(single, initial, (grads, edges, degrees))
    return result

def relation_sum(agg, layer_weights):
    return jnp.einsum('rbd,rde->be', agg.astype(jnp.float32), layer_weights.astype(jnp.float32))

def silu_slope(preact):
    logistic = jax.nn.sigmoid(preact)
    return logistic * (1.0 + preact * (1.0 - logistic))

def weight_terms(own_rows, agg, grad):
    own_term = lax.dot_general(own_rows, grad, (((0,), (0,)), ((), ())), preferred_element_type=jnp.float32)
    rel_terms = jnp.einsum('rbd,be->rde', agg.astype(jnp.float32), grad.astype(jnp.float32))
    return jnp.concatenate([own_term[None], rel_terms], axis=0)

def input_terms(grad, layer_weights):
    own_back = lax.dot_general(grad, layer_weights[0], (((1,), (1,)), ((), ())), preferred_element_type=jnp.float32)
    rel_back = jnp.einsum('be,rde->rbd', grad.astype(jnp.float32), layer_weights[1:].astype(jnp.float32))
    return (own_back, rel_back)

def sage_step(inputs, weights, first_self, first_edges, first_degree, second_self, second_edges, second_degree, cotangent):
    first_agg = aggregate(inputs, first_edges, first_degree)
    first_own = inputs[first_self]
    first_pre = jnp.dot(first_own, weights[0, 0], preferred_element_type=jnp.float32) + relation_sum(first_agg, weights[0, 1:])
    hidden = jax.nn.silu(first_pre).astype(jnp.bfloat16)
    second_agg = aggregate(hidden, second_edges, second_degree)
    second_own = hidden[second_self]
    output = jnp.dot(second_own, weights[1, 0], preferred_element_type=jnp.float32) + relation_sum(second_agg, weights[1, 1:])
    grad_top = weight_terms(second_own, second_agg, cotangent)
    own_back, rel_back = input_terms(cotangent, weights[1])
    grad_hidden = jnp.zeros((hidden.shape[0], hidden.shape[1]), jnp.float32).at[second_self].add(own_back)
    grad_hidden = grad_hidden + spread_back(rel_back, second_edges, second_degree, hidden.shape[0])
    grad_pre = (grad_hidden * silu_slope(first_pre)).astype(jnp.bfloat16)
    grad_bottom = weight_terms(first_own, first_agg, grad_pre)
    own_back, rel_back = input_terms(grad_pre, weights[0])
    grad_slots = jnp.zeros((inputs.shape[0], inputs.shape[1]), jnp.float32).at[first_self].add(own_back)
    grad_slots = grad_slots + spread_back(rel_back, first_edges, first_degree, inputs.shape[0])
    return (output.astype(jnp.bfloat16), jnp.stack([grad_bottom, grad_top]), grad_slots)

def reference(table, weights, fetch_rows, fetch_count, first_self, first_edges, first_degree, second_self, second_edges, second_degree, cotangent):
    batches = N_DP * N_TABLE

    def flatten(array):
        return array.reshape((batches,) + array.shape[2:])
    shard_rows = table.reshape(N_TABLE, ROWS_DEV, D)

    def single(carry, bundle):
        wanted, live_count, s_one, e_one, d_one, s_two, e_two, d_two, cot_rows = bundle
        slot_pos = lax.broadcasted_iota(jnp.int32, wanted.shape, 1)
        owners = lax.broadcasted_iota(jnp.int32, wanted.shape, 0)
        living = slot_pos < live_count[:, None]
        fetched = jnp.where(living[:, :, None], shard_rows[owners, wanted], jnp.zeros((), table.dtype))
        inputs = fetched.reshape(SLOTS, D)
        node_rows, grads, grad_slots = sage_step(inputs, weights, s_one, e_one, d_one, s_two, e_two, d_two, cot_rows)
        grad_slots = jnp.where(living.reshape(-1)[:, None], grad_slots, jnp.zeros((), grad_slots.dtype))
        weight_total, table_total = carry
        targets = (owners * ROWS_DEV + wanted).reshape(-1).astype(jnp.int32)
        table_total = table_total.at[targets].add(grad_slots)
        return ((weight_total + grads, table_total), node_rows)
    initial = (jnp.zeros((2, R + 1, D, D), jnp.float32), jnp.zeros((VOCAB, D), jnp.float32))
    bundles = tuple((flatten(a) for a in (fetch_rows, fetch_count, first_self, first_edges, first_degree, second_self, second_edges, second_degree, cotangent)))
    (weight_total, table_total), outputs = lax.scan(single, initial, bundles)
    node_out = outputs.reshape(N_DP, N_TABLE, B2, D)
    weight_grad = (weight_total / jnp.sqrt(jnp.float32(SEEDS))).astype(jnp.bfloat16)
    table_grad = table_total.reshape(N_TABLE, ROWS_DEV, D)
    return (node_out, weight_grad, table_grad)
```

```python
import functools
import math

import jax
import jax.numpy as jnp
from jax import lax
from jax.experimental import pallas as pl
from jax.experimental.pallas import tpu as pltpu
from jax.sharding import PartitionSpec as P

MESH = pl.DeviceIdType.MESH
VMEM = pltpu.VMEM
F32 = jnp.float32
BF16 = jnp.bfloat16


def dot(a, b, da, db):
    return lax.dot_general(a, b, (((da,), (db,)), ((), ())), preferred_element_type=F32)


def peer_on(axis, index):
    if axis == "dp":
        return (index, lax.axis_index("table"))
    return (lax.axis_index("dp"), index)


def greet(axes_sizes):
    barrier = pltpu.get_barrier_semaphore()
    total = 0
    for axis, size in axes_sizes:
        me = lax.axis_index(axis)
        for step in range(1, size):
            pl.semaphore_signal(
                barrier,
                inc=1,
                device_id=peer_on(axis, lax.rem(me + step, size)),
                device_id_type=MESH,
            )
            total += 1
    pl.semaphore_wait(barrier, total)


def pick_rows(row_numbers, height):
    shape = (height, row_numbers.shape[1])
    match = lax.broadcasted_iota(jnp.int32, shape, 0) == row_numbers
    return jnp.where(match, F32(1), F32(0)).astype(BF16)


def fetch_kernel(
    n_table, table, wanted, fetched, asked_row, asked_all, found, ssem, rsem, ssem2, rsem2
):
    me = lax.axis_index("table")
    greet((("table", n_table),))
    sends = []
    for step in range(1, n_table):
        copy = pltpu.make_async_remote_copy(
            src_ref=wanted,
            dst_ref=asked_all.at[me],
            send_sem=ssem.at[step],
            recv_sem=rsem.at[step],
            device_id=peer_on("table", lax.rem(me + step, n_table)),
            device_id_type=MESH,
        )
        copy.start()
        sends.append(copy)
    asked_all[me] = wanted[...]
    for copy in sends:
        copy.wait_recv()
    row = jnp.concatenate([asked_all[j, pl.ds(me, 1), :] for j in range(n_table)], axis=1)
    asked_row[...] = row
    selector = pick_rows(row, table.shape[0])
    found[...] = dot(selector, table[...], 0, 0).astype(BF16).reshape(found.shape)
    replies = []
    for step in range(1, n_table):
        peer = lax.rem(me + step, n_table)
        copy = pltpu.make_async_remote_copy(
            src_ref=found.at[peer],
            dst_ref=fetched.at[me],
            send_sem=ssem2.at[step],
            recv_sem=rsem2.at[step],
            device_id=peer_on("table", peer),
            device_id_type=MESH,
        )
        copy.start()
        replies.append(copy)
    fetched[me] = found[me]
    for copy in sends:
        copy.wait_send()
    for copy in replies:
        copy.wait()


def step_kernel(
    counts,
    fetched,
    weights,
    self1,
    edges1,
    degree1,
    self2,
    edges2,
    degree2,
    cot,
    node_out,
    grads,
    slot_grads,
    c1,
    c2,
    x1t,
    x2t,
    back1,
    back2,
):
    relations, fan, width1 = edges1.shape
    width2 = edges2.shape[2]
    shards, cap, feature = fetched.shape
    slots = shards * cap
    terms = relations + 1
    common = math.lcm(*range(1, fan + 1))
    inverse = F32(1.0 / common)

    live = []
    slot_pos = lax.broadcasted_iota(jnp.int32, (cap, feature), 0)
    for k in range(shards):
        live.append(slot_pos < counts[k])
    inputs = jnp.concatenate(
        [jnp.where(live[k], fetched[k].astype(F32), F32(0)) for k in range(shards)], axis=0
    ).astype(BF16)

    def fill(selector, own, edges, degree, height, width):
        spot = lax.broadcasted_iota(jnp.int32, (height, width), 0)
        selector[:, :width] = jnp.where(spot == own[...], F32(common), F32(0)).astype(BF16)
        for r in range(relations):
            deg = degree[r]
            share = F32(common) / deg.astype(F32)
            share = jnp.floor(share + F32(0.5))
            total = jnp.zeros((height, width), F32)
            for f in range(fan):
                where = jnp.where(deg > f, edges[r, f : f + 1, :], -1)
                total = total + jnp.where(spot == where, share, F32(0))
            selector[:, (r + 1) * width : (r + 2) * width] = total.astype(BF16)

    fill(c1, self1, edges1, degree1, slots, width1)
    fill(c2, self2, edges2, degree2, width1, width2)

    x1t[...] = (dot(inputs, c1[...], 0, 0) * inverse).astype(BF16)
    pre = jnp.zeros((width1, feature), F32)
    for r in range(terms):
        pre = pre + dot(x1t[:, r * width1 : (r + 1) * width1], weights[0, r], 0, 0)
    s = 1.0 / (1.0 + jnp.exp(-pre))
    hidden = (pre * s).astype(BF16)
    slope = s * (1.0 + pre * (1.0 - s))

    x2t[...] = (dot(hidden, c2[...], 0, 0) * inverse).astype(BF16)
    cot_rows = cot[...]
    out = jnp.zeros((width2, feature), F32)
    for r in range(terms):
        part = x2t[:, r * width2 : (r + 1) * width2]
        out = out + dot(part, weights[1, r], 0, 0)
        grads[1, r] = dot(part, cot_rows, 1, 0).astype(BF16)
        back2[r * width2 : (r + 1) * width2, :] = dot(cot_rows, weights[1, r], 1, 1).astype(BF16)
    node_out[...] = out.astype(BF16)

    grad_hidden = dot(c2[...], back2[...], 1, 0) * inverse
    grad_pre = (grad_hidden * slope).astype(BF16)
    for r in range(terms):
        part = x1t[:, r * width1 : (r + 1) * width1]
        grads[0, r] = dot(part, grad_pre, 1, 0).astype(BF16)
        back1[r * width1 : (r + 1) * width1, :] = dot(grad_pre, weights[0, r], 1, 1).astype(BF16)
    grad_slots = dot(c1[...], back1[...], 1, 0) * inverse
    for k in range(shards):
        block = grad_slots[k * cap : (k + 1) * cap, :]
        slot_grads[k] = jnp.where(live[k], block, F32(0)).astype(BF16)


def reduce_kernel(
    n_dp,
    n_table,
    seeds,
    slot_grads,
    asked_row,
    grads,
    table_part,
    total_out,
    returned,
    dense,
    dense_send,
    dense_recv,
    inbox,
    running,
    s_slot,
    r_slot,
    s_dp,
    r_dp,
    s_rs,
    r_rs,
    s_ag,
    r_ag,
):
    me = lax.axis_index("table")
    my_dp = lax.axis_index("dp")
    streams, chunks = grads.shape[0], grads.shape[1]
    greet((("table", n_table), ("dp", n_dp)))

    bits = [("table", 1 << b) for b in range(n_table.bit_length() - 1)]
    bits += [("dp", 1 << b) for b in range(n_dp.bit_length() - 1)]
    head, rest = bits[:1], bits[1:]
    orders = []
    for s in range(streams):
        turn = s % max(1, len(rest))
        orders.append(head + rest[turn:] + rest[:turn])
    phases = len(bits)

    def side(axis, bit):
        return lax.rem(lax.axis_index(axis) // bit, 2)

    def partner(axis, bit):
        return peer_on(axis, lax.axis_index(axis) + bit * (1 - 2 * side(axis, bit)))

    def region(p):
        return chunks - (chunks >> p)

    def current(s, p):
        return (grads, 0) if p == 0 else (running, region(p - 1))

    def scatter_copy(s, p):
        axis, bit = orders[s][p]
        half = chunks >> (p + 1)
        ref, start = current(s, p)
        return pltpu.make_async_remote_copy(
            src_ref=ref.at[s, pl.ds(start + (1 - side(axis, bit)) * half, half)],
            dst_ref=inbox.at[s, pl.ds(region(p), half)],
            send_sem=s_rs.at[s, p],
            recv_sem=r_rs.at[s, p],
            device_id=partner(axis, bit),
            device_id_type=MESH,
        )

    def base(s, p):
        place = 0
        for q in range(p):
            axis, bit = orders[s][q]
            place = place + side(axis, bit) * (chunks >> (q + 1))
        return place

    def gather_copy(s, p):
        axis, bit = orders[s][p]
        half = chunks >> (p + 1)
        spot = pl.ds(base(s, p + 1), half)
        return pltpu.make_async_remote_copy(
            src_ref=total_out.at[s, spot],
            dst_ref=total_out.at[s, spot],
            send_sem=s_ag.at[s, p],
            recv_sem=r_ag.at[s, p],
            device_id=partner(axis, bit),
            device_id_type=MESH,
        )

    slot_copies = []
    for step in range(1, n_table):
        peer = lax.rem(me + step, n_table)
        copy = pltpu.make_async_remote_copy(
            src_ref=slot_grads.at[peer],
            dst_ref=returned.at[me],
            send_sem=s_slot.at[step],
            recv_sem=r_slot.at[step],
            device_id=peer_on("table", peer),
            device_id_type=MESH,
        )
        copy.start()
        slot_copies.append(copy)
    scatters = [[scatter_copy(s, 0)] for s in range(streams)]
    for s in range(streams):
        scatters[s][0].start()

    returned[me] = slot_grads[me]
    selector = pick_rows(asked_row[...], dense.shape[0] * dense.shape[1])
    for copy in slot_copies:
        copy.wait()
    rows = returned[...].reshape(selector.shape[1], returned.shape[2])
    dense[...] = dot(selector, rows, 1, 0).reshape(dense.shape)
    dense_send[...] = dense[...].astype(BF16)
    dp_copies = []
    for step in range(1, n_dp):
        peer = lax.rem(my_dp + step, n_dp)
        copy = pltpu.make_async_remote_copy(
            src_ref=dense_send.at[peer],
            dst_ref=dense_recv.at[step],
            send_sem=s_dp.at[step],
            recv_sem=r_dp.at[step],
            device_id=peer_on("dp", peer),
            device_id_type=MESH,
        )
        copy.start()
        dp_copies.append(copy)

    scale = F32(1.0 / math.sqrt(seeds))
    for p in range(phases):
        half = chunks >> (p + 1)
        for s in range(streams):
            axis, bit = orders[s][p]
            scatters[s][p].wait_recv()
            ref, start = current(s, p)
            mine = ref[s, pl.ds(start + side(axis, bit) * half, half)].astype(F32)
            summed = mine + inbox[s, pl.ds(region(p), half)].astype(F32)
            if p < phases - 1:
                running[s, pl.ds(region(p), half)] = summed.astype(BF16)
                copy = scatter_copy(s, p + 1)
                copy.start()
                scatters[s].append(copy)
            else:
                total_out[s, pl.ds(base(s, phases), 1)] = (summed * scale).astype(BF16)
    gathers = []
    for p in reversed(range(phases)):
        for s in range(streams):
            if p < phases - 1:
                gathers[(phases - 2 - p) * streams + s].wait_recv()
            copy = gather_copy(s, p)
            copy.start()
            gathers.append(copy)

    part = dense[my_dp]
    for copy in dp_copies:
        copy.wait()
    for step in range(1, n_dp):
        part = part + dense_recv[step].astype(F32)
    table_part[...] = part

    for s in range(streams):
        gathers[(phases - 1) * streams + s].wait_recv()
        for p in range(phases):
            scatters[s][p].wait_send()
    for copy in gathers:
        copy.wait_send()


def body(
    n_dp,
    n_table,
    table,
    weights,
    fetch_rows,
    fetch_count,
    first_self,
    first_edges,
    first_degree,
    second_self,
    second_edges,
    second_degree,
    cotangent,
):
    wanted = fetch_rows[0, 0]
    shards, cap = wanted.shape
    height, feature = table.shape
    slots = shards * cap
    relations, width1, fan = first_edges.shape[2:]
    width2 = second_edges.shape[3]
    terms = relations + 1
    vmem = pl.BlockSpec(memory_space=VMEM)
    smem = pl.BlockSpec(memory_space=pltpu.SMEM)
    dma = pltpu.SemaphoreType.DMA

    fetched, asked_row = pl.pallas_call(
        functools.partial(fetch_kernel, n_table),
        out_shape=(
            jax.ShapeDtypeStruct((shards, cap, feature), BF16),
            jax.ShapeDtypeStruct((1, slots), jnp.int32),
        ),
        in_specs=[vmem] * 2,
        out_specs=(vmem, vmem),
        scratch_shapes=[
            VMEM((n_table, shards, cap), jnp.int32),
            VMEM((shards, cap, feature), BF16),
            dma((n_table,)),
            dma((n_table,)),
            dma((n_table,)),
            dma((n_table,)),
        ],
        compiler_params=pltpu.CompilerParams(collective_id=0, has_side_effects=True),
    )(table, wanted)

    node_out, grads, slot_grads = pl.pallas_call(
        step_kernel,
        out_shape=(
            jax.ShapeDtypeStruct((width2, feature), BF16),
            jax.ShapeDtypeStruct((2, terms, feature, feature), BF16),
            jax.ShapeDtypeStruct((shards, cap, feature), BF16),
        ),
        in_specs=[smem] + [vmem] * 9,
        out_specs=(vmem,) * 3,
        scratch_shapes=[
            VMEM((slots, terms * width1), BF16),
            VMEM((width1, terms * width2), BF16),
            VMEM((feature, terms * width1), BF16),
            VMEM((feature, terms * width2), BF16),
            VMEM((terms * width1, feature), BF16),
            VMEM((terms * width2, feature), BF16),
        ],
    )(
        fetch_count[0, 0],
        fetched,
        weights,
        first_self[0],
        jnp.swapaxes(first_edges[0, 0], 1, 2),
        first_degree[0, 0][:, None],
        second_self[0],
        jnp.swapaxes(second_edges[0, 0], 1, 2),
        second_degree[0, 0][:, None],
        cotangent[0, 0],
    )

    devices = n_dp * n_table
    total_rows = 2 * terms * feature
    streams = 3 if total_rows % (3 * devices) == 0 else 1
    chunk = total_rows // (streams * devices)
    phases = devices.bit_length() - 1
    pieces = (streams, devices, chunk, feature)
    table_part, total = pl.pallas_call(
        functools.partial(reduce_kernel, n_dp, n_table, width2 * devices),
        out_shape=(
            jax.ShapeDtypeStruct((height // n_dp, feature), F32),
            jax.ShapeDtypeStruct(pieces, BF16),
        ),
        in_specs=[vmem] * 3,
        out_specs=(vmem,) * 2,
        scratch_shapes=[
            VMEM((shards, cap, feature), BF16),
            VMEM((n_dp, height // n_dp, feature), F32),
            VMEM((n_dp, height // n_dp, feature), BF16),
            VMEM((n_dp, height // n_dp, feature), BF16),
            VMEM(pieces, BF16),
            VMEM(pieces, BF16),
            dma((n_table,)),
            dma((n_table,)),
            dma((n_dp,)),
            dma((n_dp,)),
            dma((streams, phases)),
            dma((streams, phases)),
            dma((streams, phases)),
            dma((streams, phases)),
        ],
        compiler_params=pltpu.CompilerParams(collective_id=1, has_side_effects=True),
    )(slot_grads, asked_row, grads.reshape(pieces))
    return (node_out[None, None], total.reshape(weights.shape), table_part[None])


def solution(mesh):
    return jax.shard_map(
        functools.partial(body, mesh.shape["dp"], mesh.shape["table"]),
        mesh=mesh,
        in_specs=(
            P("table", None),
            P(),
            P("dp", "table", None, None),
            P("dp", "table", None),
            P("dp", "table", None),
            P("dp", "table", None, None, None),
            P("dp", "table", None, None),
            P("dp", "table", None),
            P("dp", "table", None, None, None),
            P("dp", "table", None, None),
            P("dp", "table", None, None),
        ),
        out_specs=(P("dp", "table", None, None), P(), P("table", "dp", None)),
        check_vma=False,
    )
```

```python
import functools
import math

import jax
import jax.numpy as jnp
from jax import lax
from jax.experimental import pallas as pl
from jax.experimental.pallas import tpu as pltpu
from jax.sharding import PartitionSpec as P

MESH = pl.DeviceIdType.MESH
VMEM = pltpu.VMEM
F32 = jnp.float32
BF16 = jnp.bfloat16


def dot(a, b, da, db):
    return lax.dot_general(a, b, (((da,), (db,)), ((), ())), preferred_element_type=F32)


def peer_on(axis, index):
    if axis == "dp":
        return (index, lax.axis_index("table"))
    return (lax.axis_index("dp"), index)


def greet(axes_sizes):
    barrier = pltpu.get_barrier_semaphore()
    total = 0
    for axis, size in axes_sizes:
        me = lax.axis_index(axis)
        for step in range(1, size):
            pl.semaphore_signal(
                barrier,
                inc=1,
                device_id=peer_on(axis, lax.rem(me + step, size)),
                device_id_type=MESH,
            )
            total += 1
    return lambda: pl.semaphore_wait(barrier, total)


def pick_rows(row_numbers, height):
    shape = (height, row_numbers.shape[1])
    match = lax.broadcasted_iota(jnp.int32, shape, 0) == row_numbers
    return jnp.where(match, F32(1), F32(0)).astype(BF16)


def fetch_kernel(
    n_table, table, wanted, fetched, asked_row, asked_all, found, ssem, rsem, ssem2, rsem2
):
    me = lax.axis_index("table")
    greet((("table", n_table),))()
    sends = []
    for step in range(1, n_table):
        copy = pltpu.make_async_remote_copy(
            src_ref=wanted,
            dst_ref=asked_all.at[me],
            send_sem=ssem.at[step],
            recv_sem=rsem.at[step],
            device_id=peer_on("table", lax.rem(me + step, n_table)),
            device_id_type=MESH,
        )
        copy.start()
        sends.append(copy)
    asked_all[me] = wanted[...]
    for copy in sends:
        copy.wait_recv()
    row = jnp.concatenate([asked_all[j, pl.ds(me, 1), :] for j in range(n_table)], axis=1)
    asked_row[...] = row
    selector = pick_rows(row, table.shape[0])
    found[...] = dot(selector, table[...], 0, 0).astype(BF16).reshape(found.shape)
    replies = []
    for step in range(1, n_table):
        peer = lax.rem(me + step, n_table)
        copy = pltpu.make_async_remote_copy(
            src_ref=found.at[peer],
            dst_ref=fetched.at[me],
            send_sem=ssem2.at[step],
            recv_sem=rsem2.at[step],
            device_id=peer_on("table", peer),
            device_id_type=MESH,
        )
        copy.start()
        replies.append(copy)
    fetched[me] = found[me]
    for copy in sends:
        copy.wait_send()
    for copy in replies:
        copy.wait()


def step_kernel(
    n_dp,
    n_table,
    seeds,
    counts,
    fetched,
    asked_row,
    weights,
    self1,
    edges1,
    degree1,
    self2,
    edges2,
    degree2,
    cot,
    node_out,
    table_part,
    total_out,
    c1,
    c2,
    x1t,
    x2t,
    back1,
    back2,
    slot_grads,
    grads,
    returned,
    dense,
    dense_send,
    dense_recv,
    inbox,
    running,
    outgoing,
    s_slot,
    r_slot,
    s_dp,
    r_dp,
    s_rs,
    r_rs,
    s_ag,
    r_ag,
):
    entered = greet((("table", n_table), ("dp", n_dp)))
    relations, fan, width1 = edges1.shape
    width2 = edges2.shape[2]
    shards, cap, feature = fetched.shape
    slots = shards * cap
    terms = relations + 1
    common = math.lcm(*range(1, fan + 1))
    inverse = F32(1.0 / common)
    me = lax.axis_index("table")
    my_dp = lax.axis_index("dp")
    streams, chunks, chunk = grads.shape[:3]

    pair = n_table // max(1, n_table // 2)
    across = n_table // pair
    mine_pair, mine_across = lax.rem(me, pair), me // pair
    twin = (pair, mine_pair, lambda j: peer_on("table", mine_across * pair + j))
    plane = (across, mine_across, lambda j: peer_on("table", j * pair + mine_pair))
    column = (n_dp, my_dp, lambda j: peer_on("dp", j))
    orders = [(twin, column, plane) if s == 1 else (twin, plane, column) for s in range(streams)]

    def held(s, p):
        left = chunks
        for group in orders[s][:p]:
            left //= group[0]
        return left

    def region(s, p):
        return sum(held(s, q) for q in range(1, p))

    def slot(s, p, step):
        before = sum((orders[s][q][0] - 1) * held(s, q + 1) for q in range(p))
        return before + (step - 1) * held(s, p + 1)

    def base(s, p):
        place = 0
        for q in range(p):
            place = place + orders[s][q][1] * held(s, q + 1)
        return place

    started = {}

    def scatter(s, p):
        size, place, device = orders[s][p]
        part = held(s, p + 1)
        source, start = (grads, 0) if p == 0 else (outgoing, region(s, p))
        copies = []
        for step in range(1, size):
            to = lax.rem(place + step, size)
            copy = pltpu.make_async_remote_copy(
                src_ref=source.at[s, pl.ds(start + to * part, part)],
                dst_ref=inbox.at[s, pl.ds(slot(s, p, step), part)],
                send_sem=s_rs.at[s, p, step],
                recv_sem=r_rs.at[s, p, step],
                device_id=device(to),
                device_id_type=MESH,
            )
            copy.start()
            copies.append(copy)
        started["rs", s, p] = copies

    def absorb(s, p):
        size, place, device = orders[s][p]
        part = held(s, p + 1)
        source, start = (grads, 0) if p == 0 else (running, region(s, p))
        where = pl.ds(region(s, p + 1), part)
        summed = source[s, pl.ds(start + place * part, part)].astype(F32)
        for step in range(1, size):
            started["rs", s, p][step - 1].wait_recv()
            summed = summed + inbox[s, pl.ds(slot(s, p, step), part)].astype(F32)
        if p < len(orders[s]) - 1:
            running[s, where] = summed
            outgoing[s, where] = summed.astype(BF16)
            scatter(s, p + 1)
        else:
            scale = F32(1.0 / math.sqrt(seeds))
            total_out[s, pl.ds(base(s, p + 1), part)] = (summed * scale).astype(BF16)

    def gather(s, p):
        size, place, device = orders[s][p]
        spot = pl.ds(base(s, p + 1), held(s, p + 1))
        copies = []
        for step in range(1, size):
            copy = pltpu.make_async_remote_copy(
                src_ref=total_out.at[s, spot],
                dst_ref=total_out.at[s, spot],
                send_sem=s_ag.at[s, p, step],
                recv_sem=r_ag.at[s, p, step],
                device_id=device(lax.rem(place + step, size)),
                device_id_type=MESH,
            )
            copy.start()
            copies.append(copy)
        started["ag", s, p] = copies

    def keep(block, value):
        first = block * feature // chunk
        for c in range(feature // chunk):
            s, at = divmod(first + c, chunks)
            grads[s, at] = value[c * chunk : (c + 1) * chunk, :].astype(BF16)

    live = []
    slot_pos = lax.broadcasted_iota(jnp.int32, (cap, feature), 0)
    for k in range(shards):
        live.append(slot_pos < counts[k])
    inputs = jnp.concatenate(
        [jnp.where(live[k], fetched[k].astype(F32), F32(0)) for k in range(shards)], axis=0
    ).astype(BF16)

    def fill(selector, own, edges, degree, height, width):
        spot = lax.broadcasted_iota(jnp.int32, (height, width), 0)
        selector[:, :width] = jnp.where(spot == own[...], F32(common), F32(0)).astype(BF16)
        for r in range(relations):
            deg = degree[r]
            share = jnp.zeros(deg.shape, F32)
            for d in range(1, fan + 1):
                share = jnp.where(deg == d, F32(common // d), share)
            total = jnp.zeros((height, width), F32)
            for f in range(fan):
                where = jnp.where(deg > f, edges[r, f : f + 1, :], -1)
                total = total + jnp.where(spot == where, share, F32(0))
            selector[:, (r + 1) * width : (r + 2) * width] = total.astype(BF16)

    fill(c1, self1, edges1, degree1, slots, width1)
    fill(c2, self2, edges2, degree2, width1, width2)

    x1t[...] = (dot(inputs, c1[...], 0, 0) * inverse).astype(BF16)
    pre = jnp.zeros((width1, feature), F32)
    for r in range(terms):
        pre = pre + dot(x1t[:, r * width1 : (r + 1) * width1], weights[0, r], 0, 0)
    s = 1.0 / (1.0 + jnp.exp(-pre))
    hidden = (pre * s).astype(BF16)
    slope = s * (1.0 + pre * (1.0 - s))

    x2t[...] = (dot(hidden, c2[...], 0, 0) * inverse).astype(BF16)
    cot_rows = cot[...]
    for r in range(terms):
        part = x2t[:, r * width2 : (r + 1) * width2]
        keep(terms + r, dot(part, cot_rows, 1, 0))
    early = [n for n in range(streams) if n * chunks * chunk >= terms * feature]
    late = [n for n in reversed(range(streams)) if n not in early]
    entered()
    for n in early:
        scatter(n, 0)

    for r in range(terms):
        back2[r * width2 : (r + 1) * width2, :] = dot(cot_rows, weights[1, r], 1, 1).astype(BF16)
    grad_hidden = dot(c2[...], back2[...], 1, 0) * inverse
    grad_pre = (grad_hidden * slope).astype(BF16)
    for r in range(terms):
        part = x1t[:, r * width1 : (r + 1) * width1]
        keep(r, dot(part, grad_pre, 1, 0))
    for n in late:
        scatter(n, 0)
    for n in early:
        absorb(n, 0)

    for r in range(terms):
        back1[r * width1 : (r + 1) * width1, :] = dot(grad_pre, weights[0, r], 1, 1).astype(BF16)
    grad_slots = dot(c1[...], back1[...], 1, 0) * inverse
    for k in range(shards):
        block = grad_slots[k * cap : (k + 1) * cap, :]
        slot_grads[k] = jnp.where(live[k], block, F32(0)).astype(BF16)
    slot_copies = []
    for step in range(1, n_table):
        peer = lax.rem(me + step, n_table)
        copy = pltpu.make_async_remote_copy(
            src_ref=slot_grads.at[peer],
            dst_ref=returned.at[me],
            send_sem=s_slot.at[step],
            recv_sem=r_slot.at[step],
            device_id=peer_on("table", peer),
            device_id_type=MESH,
        )
        copy.start()
        slot_copies.append(copy)
    returned[me] = slot_grads[me]
    for n in late:
        absorb(n, 0)

    out = jnp.zeros((width2, feature), F32)
    for r in range(terms):
        out = out + dot(x2t[:, r * width2 : (r + 1) * width2], weights[1, r], 0, 0)
    node_out[...] = out.astype(BF16)
    selector = pick_rows(asked_row[...], dense.shape[0] * dense.shape[1])
    for copy in slot_copies:
        copy.wait()
    rows = returned[...].reshape(selector.shape[1], feature)
    dense[...] = dot(selector, rows, 1, 0).reshape(dense.shape)
    dense_send[...] = dense[...].astype(BF16)
    dp_copies = []
    for step in range(1, n_dp):
        peer = lax.rem(my_dp + step, n_dp)
        copy = pltpu.make_async_remote_copy(
            src_ref=dense_send.at[peer],
            dst_ref=dense_recv.at[step],
            send_sem=s_dp.at[step],
            recv_sem=r_dp.at[step],
            device_id=peer_on("dp", peer),
            device_id_type=MESH,
        )
        copy.start()
        dp_copies.append(copy)

    turn = early + late
    for n in turn:
        absorb(n, 1)
    for n in turn:
        absorb(n, 2)
        gather(n, 2)
    shard = dense[my_dp]
    for copy in dp_copies:
        copy.wait()
    for step in range(1, n_dp):
        shard = shard + dense_recv[step].astype(F32)
    table_part[...] = shard
    for p in (1, 0):
        for n in turn:
            for copy in started["ag", n, p + 1]:
                copy.wait_recv()
            gather(n, p)
    for n in turn:
        for copy in started["ag", n, 0]:
            copy.wait_recv()
        for p in range(3):
            for copy in started["rs", n, p] + started["ag", n, p]:
                copy.wait_send()


def body(
    n_dp,
    n_table,
    table,
    weights,
    fetch_rows,
    fetch_count,
    first_self,
    first_edges,
    first_degree,
    second_self,
    second_edges,
    second_degree,
    cotangent,
):
    wanted = fetch_rows[0, 0]
    shards, cap = wanted.shape
    height, feature = table.shape
    slots = shards * cap
    relations, width1, fan = first_edges.shape[2:]
    width2 = second_edges.shape[3]
    terms = relations + 1
    vmem = pl.BlockSpec(memory_space=VMEM)
    smem = pl.BlockSpec(memory_space=pltpu.SMEM)
    dma = pltpu.SemaphoreType.DMA

    fetched, asked_row = pl.pallas_call(
        functools.partial(fetch_kernel, n_table),
        out_shape=(
            jax.ShapeDtypeStruct((shards, cap, feature), BF16),
            jax.ShapeDtypeStruct((1, slots), jnp.int32),
        ),
        in_specs=[vmem] * 2,
        out_specs=(vmem, vmem),
        scratch_shapes=[
            VMEM((n_table, shards, cap), jnp.int32),
            VMEM((shards, cap, feature), BF16),
            dma((n_table,)),
            dma((n_table,)),
            dma((n_table,)),
            dma((n_table,)),
        ],
        compiler_params=pltpu.CompilerParams(collective_id=0, has_side_effects=True),
    )(table, wanted)

    devices = n_dp * n_table
    total_rows = 2 * terms * feature
    streams = 3 if total_rows % (3 * devices) == 0 else 1
    chunk = total_rows // (streams * devices)
    pieces = (streams, devices, chunk, feature)
    widest = max(2, n_table // 2, n_dp)
    ways = (streams, 3, widest)
    node_out, table_part, total = pl.pallas_call(
        functools.partial(step_kernel, n_dp, n_table, width2 * devices),
        out_shape=(
            jax.ShapeDtypeStruct((width2, feature), BF16),
            jax.ShapeDtypeStruct((height // n_dp, feature), F32),
            jax.ShapeDtypeStruct(pieces, BF16),
        ),
        in_specs=[smem] + [vmem] * 10,
        out_specs=(vmem,) * 3,
        scratch_shapes=[
            VMEM((slots, terms * width1), BF16),
            VMEM((width1, terms * width2), BF16),
            VMEM((feature, terms * width1), BF16),
            VMEM((feature, terms * width2), BF16),
            VMEM((terms * width1, feature), BF16),
            VMEM((terms * width2, feature), BF16),
            VMEM((shards, cap, feature), BF16),
            VMEM(pieces, BF16),
            VMEM((shards, cap, feature), BF16),
            VMEM((n_dp, height // n_dp, feature), F32),
            VMEM((n_dp, height // n_dp, feature), BF16),
            VMEM((n_dp, height // n_dp, feature), BF16),
            VMEM(pieces, BF16),
            VMEM(pieces, F32),
            VMEM(pieces, BF16),
            dma((n_table,)),
            dma((n_table,)),
            dma((n_dp,)),
            dma((n_dp,)),
            dma(ways),
            dma(ways),
            dma(ways),
            dma(ways),
        ],
        compiler_params=pltpu.CompilerParams(collective_id=1, has_side_effects=True),
    )(
        fetch_count[0, 0],
        fetched,
        asked_row,
        weights,
        first_self[0],
        jnp.swapaxes(first_edges[0, 0], 1, 2),
        first_degree[0, 0][:, None],
        second_self[0],
        jnp.swapaxes(second_edges[0, 0], 1, 2),
        second_degree[0, 0][:, None],
        cotangent[0, 0],
    )
    return (node_out[None, None], total.reshape(weights.shape), table_part[None])


def solution(mesh):
    return jax.shard_map(
        functools.partial(body, mesh.shape["dp"], mesh.shape["table"]),
        mesh=mesh,
        in_specs=(
            P("table", None),
            P(),
            P("dp", "table", None, None),
            P("dp", "table", None),
            P("dp", "table", None),
            P("dp", "table", None, None, None),
            P("dp", "table", None, None),
            P("dp", "table", None),
            P("dp", "table", None, None, None),
            P("dp", "table", None, None),
            P("dp", "table", None, None),
        ),
        out_specs=(P("dp", "table", None, None), P(), P("table", "dp", None)),
        check_vma=False,
    )
```
